32 devices in a mesh: row: 4 (over y, core), col: 8 (over z, x).
Axes of the slice: x: 2, y: 2, z: 4, core: 2. Of those that a mesh axis runs over, the one named last changes fastest.
Arguments:
- l_saved: bfloat16 [16, 4, 256, 8, 256], P(None, 'row', None, 'col'), as said below
- l_grad: bfloat16 [16, 4, 256, 8, 256], P(None, 'row', None, 'col'), as said below
Outputs:
- grad_out: float32 [16, 4, 256, 8, 256], P(None, 'row', None, 'col')
Inputs may be any that keep to these rules, and one draw needn't show every extreme that they name: Read as one matrix of 16384 rows, l_saved is lower triangular with its diagonal between 1 and 2. Read as one matrix, l_grad is zero above the diagonal.
All inputs are finite; a program needn't handle non-finite values.
Results may differ from the reference program's by a relative error of at most 0.0003.
Values may be sent and summed in bfloat16 or wider, within the bound.
A program may use at most 64 MiB of HBM per device.

```python
import jax
import jax.numpy as jnp
from jax import lax

TILE = 256
N = 16384
TR = 16
N_ROW = 4
N_COL = 8


def global_index(shape):
    tile_row = lax.broadcasted_iota(jnp.int32, shape, 0) * N_ROW + lax.broadcasted_iota(jnp.int32, shape, 1)
    rows = tile_row * TILE + lax.broadcasted_iota(jnp.int32, shape, 2)
    cols = lax.broadcasted_iota(jnp.int32, shape, 3) * TILE + lax.broadcasted_iota(jnp.int32, shape, 4)
    return (rows, cols)


def draw_l_saved(key, part):
    shape = (TR, N_ROW, TILE, N_COL, TILE)
    rows, cols = global_index(shape)
    first, second = jax.random.split(jax.random.fold_in(key, 11))
    base = jax.random.normal(first, shape, jnp.float32)
    same_tile = rows // TILE == cols // TILE
    spread = jnp.where(same_tile, 0.35 / TILE ** 0.5, (N * TILE) ** (-0.25))
    diagonal = jax.random.uniform(second, shape, jnp.float32, 1.0, 2.0)
    value = jnp.where(rows > cols, base * spread, jnp.where(rows == cols, diagonal, 0.0))
    return value.astype(jnp.bfloat16)


def draw_l_grad(key, part):
    shape = (TR, N_ROW, TILE, N_COL, TILE)
    rows, cols = global_index(shape)
    first = jax.random.fold_in(jax.random.fold_in(key, 23), 0)
    base = jax.random.normal(first, shape, jnp.float32)
    return jnp.where(rows >= cols, base, 0.0).astype(jnp.bfloat16)


def setup_inputs(seed: int = 0) -> dict:
    seeds = jax.random.split(jax.random.key(seed), 3)
    l_saved = draw_l_saved(jax.random.fold_in(seeds[2], 71), 0)
    l_grad = draw_l_grad(jax.random.fold_in(seeds[2], 71), 0)
    return dict(l_saved=l_saved, l_grad=l_grad)


HIGH = lax.Precision.HIGHEST

def right_solve(factor, rhs):
    return lax.linalg.triangular_solve(factor, rhs, left_side=False, lower=True)

def diag_gradient(factor, lower_part):
    eye = jnp.eye(factor.shape[0], dtype=jnp.float32)
    middle = jnp.dot(factor.T.astype(jnp.float32), lower_part.astype(jnp.float32), precision=HIGH, preferred_element_type=jnp.float32)
    middle = jnp.tril(middle) - 0.5 * middle * eye
    half = lax.linalg.triangular_solve(factor, middle, left_side=True, lower=True, transpose_a=True)
    full = right_solve(factor, half)
    return full + full.T

def stacked_inner(left, right):
    flat_left = left.reshape(-1, left.shape[-1])
    flat_right = right.reshape(-1, right.shape[-1]).astype(jnp.float32)
    return lax.dot_general(flat_left.astype(jnp.float32), flat_right.astype(jnp.float32), (((0,), (0,)), ((), ())), precision=HIGH, preferred_element_type=jnp.float32)

def reference(l_saved, l_grad):
    n_tiles = N // TILE
    n_cols = N_COL
    factor = l_saved.reshape(n_tiles, TILE, n_cols, TILE).transpose(0, 2, 1, 3)
    grad = l_grad.reshape(n_tiles, TILE, n_cols, TILE).transpose(0, 2, 1, 3).astype(jnp.float32)
    tile_ids = jnp.arange(n_tiles, dtype=jnp.int32)
    col_ids = jnp.arange(n_cols, dtype=jnp.int32)
    eye = jnp.eye(TILE, dtype=jnp.float32)
    for panel in (n_cols - 1, n_cols - 2):
        diag_factor = factor[panel, panel].astype(jnp.float32)
        inverse = right_solve(diag_factor, eye)
        below = (tile_ids > panel)[:, None, None]
        column = grad[:, panel]
        solved = jnp.dot(column.reshape(-1, TILE).astype(jnp.float32), inverse.astype(jnp.float32), precision=HIGH, preferred_element_type=jnp.float32).reshape(n_tiles, TILE, TILE)
        cbar = jnp.where(below, solved, jnp.float32(0.0))
        total = column[panel] - stacked_inner(cbar, factor[:, panel])
        sym = diag_gradient(diag_factor, jnp.tril(total))

        def one_column(kcol):
            row_factor = factor[panel, kcol].astype(jnp.float32)
            update = jnp.dot(cbar.reshape(-1, TILE).astype(jnp.float32), row_factor.astype(jnp.float32), precision=HIGH, preferred_element_type=jnp.float32)
            fresh = grad[:, kcol] - update.reshape(n_tiles, TILE, TILE)
            summed = stacked_inner(cbar, factor[:, kcol])
            own = grad[panel, kcol] - (summed + jnp.dot(sym.astype(jnp.float32), row_factor.astype(jnp.float32), precision=HIGH, preferred_element_type=jnp.float32))
            return fresh.at[panel].set(own)
        updated = lax.map(one_column, col_ids).transpose(1, 0, 2, 3)
        abar = jnp.tril(sym) - 0.5 * sym * eye
        panel_col = jnp.where(below, cbar, jnp.where((tile_ids == panel)[:, None, None], abar[None], jnp.float32(0.0)))
        grad = jnp.where((col_ids < panel)[None, :, None, None], updated, grad)
        grad = grad.at[:, panel].set(panel_col)
    return grad.transpose(0, 2, 1, 3).reshape(TR, N_ROW, TILE, N_COL, TILE)
```

```python
import jax
import jax.numpy as jnp
from jax import lax
from jax.sharding import PartitionSpec as P

F32 = jnp.float32
BF16 = jnp.bfloat16
HIGH3 = lax.Precision.HIGH


def dot3(a, b, ca=1, cb=0):
    return lax.dot_general(
        a, b, (((ca,), (cb,)), ((), ())), precision=HIGH3, preferred_element_type=F32
    )


def bdot(a, b):
    return lax.dot_general(
        a, b, (((2,), (1,)), ((0,), (0,))), precision=HIGH3, preferred_element_type=F32
    )


def inverse_pair(tiles):
    tile = tiles.shape[-1]
    rows = lax.broadcasted_iota(jnp.int32, (tile, tile), 0)
    cols = lax.broadcasted_iota(jnp.int32, (tile, tile), 1)
    eye = (rows == cols).astype(F32)
    recip = 1.0 / jnp.sum(tiles * eye, axis=2)
    inv = eye * recip[:, None, :]
    size = 1
    while size < tile:
        off = (rows // size % 2 == 1) & (cols // size == rows // size - 1)
        part = jnp.where(off, tiles, 0.0)
        if size == 1:
            inv = inv - recip[:, :, None] * part * recip[:, None, :]
        else:
            inv = inv - bdot(inv, bdot(part, inv))
        size *= 2
    return inv


def per_device(l_saved, l_grad):
    rows_here, tile = l_saved.shape[0], l_saved.shape[2]
    n_row = lax.axis_size("row")
    n_col = lax.axis_size("col")
    factor = l_saved.reshape(rows_here, tile, tile)
    grad = l_grad.reshape(rows_here, tile, tile)
    my_row = lax.axis_index("row")
    my_col = lax.axis_index("col")
    assert n_col % n_row == 0
    first = n_col // n_row
    loc = first - 1
    lo, hi = n_col - 2, n_col - 1

    l_dk = lax.all_gather(factor[loc], "row")[n_row - 2 :].reshape(2 * tile, tile)
    mine = jnp.concatenate([l_dk, grad[first:].reshape(-1, tile)], 0)
    zero = jnp.zeros_like(mine)
    both = jnp.concatenate(
        [jnp.where(my_col == lo, mine, zero), jnp.where(my_col == hi, mine, zero)], 1
    )
    both = lax.psum(both, "col")
    l_dd = both[: 2 * tile].astype(F32)
    g_d = both[2 * tile :]

    l66, l76, l77 = l_dd[:tile, :tile], l_dd[tile:, :tile], l_dd[tile:, tile:]
    inv = inverse_pair(jnp.stack([l66, l77]))
    w76 = -dot3(inv[1], dot3(l76, inv[0]))
    w = jnp.concatenate(
        [
            jnp.concatenate([inv[0], jnp.zeros_like(w76)], 1),
            jnp.concatenate([w76, inv[1]], 1),
        ],
        0,
    )

    below_l = factor[first:].reshape(-1, tile)
    h = lax.dot_general(g_d, below_l, (((0,), (0,)), ((), ())), preferred_element_type=F32)
    t = dot3(w, lax.psum(h, "row"), 0, 0)

    fresh = grad[loc].astype(F32)
    g_dk = lax.all_gather(grad[loc], "row")[n_row - 2 :].reshape(2 * tile, tile).astype(F32)
    q_mine = g_dk - t
    z2 = jnp.zeros_like(q_mine)
    q = lax.psum(
        jnp.concatenate([jnp.where(my_col == lo, q_mine, z2), jnp.where(my_col == hi, q_mine, z2)], 1),
        "col",
    )
    eye2 = jnp.eye(2 * tile, dtype=F32)
    q = jnp.tril(q)
    m = dot3(l_dd, q, 0, 0)
    phi = jnp.tril(m) - 0.5 * m * eye2
    half = dot3(dot3(w, phi, 0, 0), w)
    s = half + half.T
    out_dd = jnp.tril(s) - 0.5 * s * eye2

    right = my_col >= lo
    w_mine = jnp.where(my_col == lo, w[:, :tile], w[:, tile:])
    x = jnp.where(right, -w_mine, dot3(w, l_dk.astype(F32)))
    x_hi = lax.reduce_precision(x, 8, 7)
    x_lo = (x - x_hi).astype(BF16)
    x_hi = x_hi.astype(BF16)
    prod = jnp.dot(g_d, x_hi, preferred_element_type=F32) + jnp.dot(
        g_d, x_lo, preferred_element_type=F32
    )
    base = jnp.where(right, jnp.zeros((), BF16), grad[first:]).astype(F32)
    low = base - prod.reshape(-1, tile, tile)

    at_lo = my_row == n_row - 2
    s_row = jnp.where(at_lo, s[:tile], s[tile:])
    t_row = jnp.where(at_lo, t[:tile], t[tile:])
    own = fresh - (t_row + dot3(s_row, l_dk.astype(F32)))
    d_row = jnp.where(at_lo, out_dd[:tile], out_dd[tile:])
    d_own = jnp.where(my_col == lo, d_row[:, :tile], d_row[:, tile:])
    in_panel = my_row >= n_row - 2
    zt = jnp.zeros_like(fresh)
    own = jnp.where(
        in_panel, jnp.where(right, d_own, own), jnp.where(right, zt, fresh)
    )
    upper = jnp.where(right, jnp.zeros((), BF16), grad[:loc]).astype(F32)
    out = jnp.concatenate([upper, own[None], low], 0)
    return out.reshape(l_grad.shape)


def solution(mesh):
    spec = P(None, "row", None, "col", None)
    return jax.shard_map(
        per_device, mesh=mesh, in_specs=(spec, spec), out_specs=spec, check_vma=False
    )
```

```python
import functools

import jax
import jax.numpy as jnp
from jax import lax
from jax.experimental import pallas as pl
from jax.experimental.pallas import tpu as pltpu
from jax.sharding import PartitionSpec as P

F32 = jnp.float32
BF16 = jnp.bfloat16
HIGH3 = lax.Precision.HIGH


def dot3(a, b, ca=1, cb=0):
    return lax.dot_general(
        a, b, (((ca,), (cb,)), ((), ())), precision=HIGH3, preferred_element_type=F32
    )


def bdot(a, b):
    return lax.dot_general(
        a, b, (((2,), (1,)), ((0,), (0,))), precision=HIGH3, preferred_element_type=F32
    )


def inverse_pair(tiles):
    tile = tiles.shape[-1]
    rows = lax.broadcasted_iota(jnp.int32, (tile, tile), 0)
    cols = lax.broadcasted_iota(jnp.int32, (tile, tile), 1)
    eye = (rows == cols).astype(F32)
    recip = 1.0 / jnp.sum(tiles * eye, axis=2)
    inv = eye * recip[:, None, :]
    size = 1
    while size < tile:
        off = (rows // size % 2 == 1) & (cols // size == rows // size - 1)
        part = jnp.where(off, tiles, 0.0)
        if size == 1:
            inv = inv - recip[:, :, None] * part * recip[:, None, :]
        else:
            inv = inv - bdot(inv, bdot(part, inv))
        size *= 2
    return inv


def spread_kernel(n_col, in_ref, out_ref, send_sem, recv_sem):
    n = in_ref.shape[0]
    ring = n_col // 2
    col = lax.axis_index("col")
    q, p = col // 2, col % 2
    up = lax.rem(q + 1, ring) * 2 + p
    down = lax.rem(q + ring - 1, ring) * 2 + p
    twin = 2 * q + 1 - p

    barrier = pltpu.get_barrier_semaphore()
    for peer in (up, down, twin):
        pl.semaphore_signal(barrier, inc=1, device_id={"col": peer}, device_id_type=pl.DeviceIdType.MESH)
    pl.semaphore_wait(barrier, 3)

    k_of = (lax.rem(q + 1, ring), ring - 1 - q)
    nexts = (up, down)
    backs = (down, up)
    streams = [(s, d) for s in (0, 1) for d in (0, 1)]

    def copy(src, s, t, slot, dev):
        return pltpu.make_async_remote_copy(
            src_ref=src.at[t],
            dst_ref=out_ref.at[s, t],
            send_sem=send_sem.at[s, t, slot],
            recv_sem=recv_sem.at[s, t],
            device_id={"col": dev},
            device_id_type=pl.DeviceIdType.MESH,
        )

    def roles(s, d, idx):
        k = k_of[d]
        main = p == s
        once = idx % 3 == 0
        source = main & (k == 0)
        fwd = (main | once) & (k < ring - 1)
        cross = main & jnp.where(once, k == 0, k > 0)
        back = jnp.logical_not(once) & jnp.logical_not(main) & (k == 1)
        return source, fwd, cross, back

    half = (n + 1) // 2

    def step(j, _):
        for s, d in streams:
            lag = k_of[d] + jnp.where(p == s, 0, 1)
            idx = j - lag
            t = 2 * idx + d
            live = (idx >= 0) & (t < n)
            source, fwd, cross, back = roles(s, d, idx)
            moves = fwd | cross | back

            @pl.when(live & source)
            def _():
                @pl.when(fwd)
                def _():
                    copy(in_ref, s, t, 0, nexts[d]).start()

                @pl.when(cross)
                def _():
                    copy(in_ref, s, t, 1, twin).start()

            @pl.when(live & moves & jnp.logical_not(source))
            def _():
                copy(out_ref.at[s], s, t, 0, twin).wait_recv()

                @pl.when(fwd)
                def _():
                    copy(out_ref.at[s], s, t, 0, nexts[d]).start()

                @pl.when(cross)
                def _():
                    copy(out_ref.at[s], s, t, 1, twin).start()

                @pl.when(back)
                def _():
                    copy(out_ref.at[s], s, t, 0, backs[d]).start()

        return 0

    lax.fori_loop(0, half + ring + 1, step, 0)

    for s in (0, 1):

        @pl.when(col == n_col - 2 + s)
        def _():
            def keep(t, _):
                out_ref[s, t] = in_ref[t]
                return 0

            lax.fori_loop(0, n, keep, 0)

    def finish(idx, _):
        for s, d in streams:
            t = 2 * idx + d
            live = t < n
            source, fwd, cross, back = roles(s, d, idx)
            moves = fwd | cross | back

            @pl.when(live & jnp.logical_not(moves) & jnp.logical_not(source))
            def _():
                copy(out_ref.at[s], s, t, 0, twin).wait_recv()

            @pl.when(live & (fwd | back))
            def _():
                copy(out_ref.at[s], s, t, 0, twin).wait_send()

            @pl.when(live & cross)
            def _():
                copy(out_ref.at[s], s, t, 1, twin).wait_send()

        return 0

    lax.fori_loop(0, half, finish, 0)


def spread(mine, n_col):
    n, tile = mine.shape[0], mine.shape[1]
    vmem = pl.BlockSpec(memory_space=pltpu.VMEM)
    return pl.pallas_call(
        functools.partial(spread_kernel, n_col),
        out_shape=jax.ShapeDtypeStruct((2, n, tile, tile), mine.dtype),
        in_specs=[vmem],
        out_specs=vmem,
        scratch_shapes=[pltpu.SemaphoreType.DMA((2, n, 2)), pltpu.SemaphoreType.DMA((2, n))],
        compiler_params=pltpu.CompilerParams(collective_id=0, has_side_effects=True),
        name="spread",
    )(mine)


def per_device(l_saved, l_grad):
    rows_here, tile = l_saved.shape[0], l_saved.shape[2]
    n_row = lax.axis_size("row")
    n_col = lax.axis_size("col")
    factor = l_saved.reshape(rows_here, tile, tile)
    grad = l_grad.reshape(rows_here, tile, tile)
    my_row = lax.axis_index("row")
    my_col = lax.axis_index("col")
    assert n_col % n_row == 0
    first = n_col // n_row
    loc = first - 1
    lo, hi = n_col - 2, n_col - 1

    l_rows = lax.all_gather(factor[loc], "row")[n_row - 2 :]
    l_dk = l_rows.reshape(2 * tile, tile)
    both = spread(jnp.concatenate([l_rows, grad[first:]], 0), n_col)
    l_dd = jnp.concatenate([both[i, :2].reshape(2 * tile, tile) for i in (0, 1)], 1).astype(F32)
    g_lo = both[0, 2:].reshape(-1, tile)
    g_hi = both[1, 2:].reshape(-1, tile)

    l66, l76, l77 = l_dd[:tile, :tile], l_dd[tile:, :tile], l_dd[tile:, tile:]
    inv = inverse_pair(jnp.stack([l66, l77]))
    w76 = -dot3(inv[1], dot3(l76, inv[0]))
    w = jnp.concatenate(
        [
            jnp.concatenate([inv[0], jnp.zeros_like(w76)], 1),
            jnp.concatenate([w76, inv[1]], 1),
        ],
        0,
    )

    below_l = factor[first:].reshape(-1, tile)
    h = jnp.concatenate(
        [
            lax.dot_general(g, below_l, (((0,), (0,)), ((), ())), preferred_element_type=F32)
            for g in (g_lo, g_hi)
        ],
        0,
    )
    t = dot3(w, lax.psum(h, "row"), 0, 0)

    fresh = grad[loc].astype(F32)
    g_dk = lax.all_gather(grad[loc], "row")[n_row - 2 :].reshape(2 * tile, tile).astype(F32)
    q_mine = g_dk - t
    z2 = jnp.zeros_like(q_mine)
    q = lax.psum(
        jnp.concatenate([jnp.where(my_col == lo, q_mine, z2), jnp.where(my_col == hi, q_mine, z2)], 1),
        "col",
    )
    eye2 = jnp.eye(2 * tile, dtype=F32)
    q = jnp.tril(q)
    m = dot3(l_dd, q, 0, 0)
    phi = jnp.tril(m) - 0.5 * m * eye2
    half = dot3(dot3(w, phi, 0, 0), w)
    s = half + half.T
    out_dd = jnp.tril(s) - 0.5 * s * eye2

    right = my_col >= lo
    w_mine = jnp.where(my_col == lo, w[:, :tile], w[:, tile:])
    x = jnp.where(right, -w_mine, dot3(w, l_dk.astype(F32)))
    x_hi = lax.reduce_precision(x, 8, 7)
    x_lo = (x - x_hi).astype(BF16)
    x_hi = x_hi.astype(BF16)
    prod = sum(
        jnp.dot(g, part[i * tile : (i + 1) * tile], preferred_element_type=F32)
        for part in (x_lo, x_hi)
        for i, g in enumerate((g_lo, g_hi))
    )
    base = jnp.where(right, jnp.zeros((), BF16), grad[first:]).astype(F32)
    low = base - prod.reshape(-1, tile, tile)

    at_lo = my_row == n_row - 2
    s_row = jnp.where(at_lo, s[:tile], s[tile:])
    t_row = jnp.where(at_lo, t[:tile], t[tile:])
    own = fresh - (t_row + dot3(s_row, l_dk.astype(F32)))
    d_row = jnp.where(at_lo, out_dd[:tile], out_dd[tile:])
    d_own = jnp.where(my_col == lo, d_row[:, :tile], d_row[:, tile:])
    in_panel = my_row >= n_row - 2
    zt = jnp.zeros_like(fresh)
    own = jnp.where(
        in_panel, jnp.where(right, d_own, own), jnp.where(right, zt, fresh)
    )
    upper = jnp.where(right, jnp.zeros((), BF16), grad[:loc]).astype(F32)
    out = jnp.concatenate([upper, own[None], low], 0)
    return out.reshape(l_grad.shape)


def solution(mesh):
    spec = P(None, "row", None, "col", None)
    return jax.shard_map(
        per_device, mesh=mesh, in_specs=(spec, spec), out_specs=spec, check_vma=False
    )
```
